256 devices in a mesh: rep: 2 (over x_hi), shard: 128 (over z, x_lo, y, core).
Axes of the slice: x: 4 (x_hi: 2, x_lo: 2; x = x_hi * 2 + x_lo), y: 4, z: 8, core: 2. Of those that a mesh axis runs over, the one named last changes fastest.
Arguments:
- tokens_x: bfloat16 [65536, 4096], P(('rep', 'shard')), may hold values from -24 to 24
- key_grad: bfloat16 [65536, 1024], P(('rep', 'shard')), may hold values from -0.0234375 to 0.0234375
- left_root: bfloat16 [512, 512, 512], P('shard'), may hold values from -1 to 3
- slot_grads: bfloat16 [512, 512, 512], P('shard'), may hold values from -6 to 6
- right_root: bfloat16 [512, 512, 512], P('shard'), may hold values from -1 to 3
- block_slot: int32 [256], replicated, may hold values from 0 to 511, as said below
Outputs:
- grad_key: float32 [4096, 1024], P('shard')
- update: bfloat16 [512, 256, 512], P('shard')
The draws below stay inside these ranges and needn't reach their ends.
Inputs may be any that keep to these rules, and one draw needn't show every extreme that they name: `block_slot`: the entries are distinct; slot v is slot v % 4 of shard index v // 4; no shard index holds more than 4 blocks, and some shard index holds exactly 4.
All inputs are finite; a program needn't handle non-finite values.
Results may differ from the reference program's by a relative error of at most 0.006.
Values may be sent and summed in bfloat16 or wider, within the bound.
A program may use at most 128 MiB of HBM per device.

```python
import jax
import jax.numpy as jnp
from jax import lax

D = 4096
KEY_WIDTH = 1024
TOK_DEV = 256
BLOCK = 512
SLOTS = 4
NBLK = 256
SLOT_ALL = 512
TOKENS = 65536


def root_matrix(key):
    first_key, second_key = jax.random.split(key)
    diagonal = jnp.exp(jax.random.uniform(first_key, (SLOT_ALL, BLOCK), jnp.float32, jnp.log(0.5), jnp.log(2.0)))
    noise = jax.random.normal(second_key, (SLOT_ALL, BLOCK, BLOCK), jnp.float32)
    symmetric = (noise + jnp.swapaxes(noise, 1, 2)) * (0.5 / (2.0 * BLOCK) ** 0.5)
    symmetric = jnp.clip(symmetric, -0.9, 0.9)
    identity = jnp.eye(BLOCK, dtype=jnp.float32)
    return (symmetric + diagonal[:, :, None] * identity[None, :, :]).astype(jnp.bfloat16)


def draw_left_root(key, part):
    return root_matrix(jax.random.fold_in(key, 11))


def draw_right_root(key, part):
    return root_matrix(jax.random.fold_in(key, 23))


def draw_block_slot(key, part):
    base_key = jax.random.fold_in(key, 37)
    first_key, second_key, third_key = jax.random.split(base_key, 3)
    full_owner = jax.random.randint(first_key, (), 0, SLOT_ALL // SLOTS)
    slot_ids = jnp.arange(SLOT_ALL, dtype=jnp.int32)
    ranking = jax.random.permutation(second_key, SLOT_ALL).astype(jnp.int32)
    ranking = jnp.where(slot_ids // SLOTS == full_owner, slot_ids % SLOTS - SLOTS, ranking)
    chosen = jnp.argsort(ranking, stable=True)[:NBLK].astype(jnp.int32)
    shuffled = jax.random.permutation(third_key, NBLK).astype(jnp.int32)
    return chosen[shuffled].astype(jnp.int32)


def strengthened(array, rng, source, target, parts, factor):
    def block_of(position):
        return (jnp.arange(array.shape[position]) // (array.shape[position] // parts)).reshape((-1,) + (1,) * (array.ndim - 1 - position))

    near = jax.random.permutation(rng, parts)[block_of(target)]
    second = (block_of(target) + parts // 2) % parts
    return jnp.where((block_of(source) == near) | (block_of(source) == second), factor * array, array)


def block_levels(own_key, shape, cuts, least, top_value):
    gain, own = 1.0, jax.random.fold_in(own_key, 6)
    for axis_at, shards_of in cuts:
        draws = jnp.exp(jax.random.uniform(jax.random.fold_in(own, axis_at), (shards_of,), jnp.float32, least / len(cuts), top_value / len(cuts)))
        gain = gain * jnp.repeat(draws, shape[axis_at] // shards_of).reshape([-1 if axis == axis_at else 1 for axis in range(len(shape))])
    return gain


def normal_values(rng, dims, scale, reach, cuts=(), kind=jnp.bfloat16):
    entries = jax.random.normal(rng, dims, jnp.float32) * scale
    if len(cuts) > 0:
        entries = block_levels(rng, dims, cuts, -0.22, 0.18) * entries
    return jnp.clip(entries, min=-reach, max=reach).astype(kind)


def noise_with(stream_key, extent, spread, reach, cuts, heavy, kind=jnp.bfloat16):
    drawn = spread * jax.random.normal(stream_key, extent, jnp.float32)
    if cuts:
        drawn = drawn * block_levels(stream_key, extent, cuts, -0.22, 0.18)
    return jnp.clip(strengthened(drawn, jax.random.fold_in(stream_key, 3), *heavy), -reach, reach).astype(kind)


def setup_inputs(seed: int = 0) -> dict:
    keys = jax.random.split(jax.random.key(seed), 7)
    return {
        "tokens_x": noise_with(keys[0], (TOKENS, D), 1.0, 24.0, ((0, 256),), (0, 1, 256, 6.0)),
        "key_grad": normal_values(keys[1], (TOKENS, KEY_WIDTH), (TOKENS ** -0.5), 0.0234375, ((0, 256),)),
        "left_root": draw_left_root(jax.random.fold_in(keys[6], 71), 0),
        "slot_grads": normal_values(keys[3], (SLOT_ALL, BLOCK, BLOCK), 1.0, 6.0, ((0, 128),)),
        "right_root": draw_right_root(jax.random.fold_in(keys[6], 71), 0),
        "block_slot": draw_block_slot(jax.random.fold_in(keys[6], 71), 0),
    }


def reference(tokens_x, key_grad, left_root, slot_grads, right_root, block_slot):
    step_count = TOKENS // TOK_DEV
    token_blocks = tokens_x.reshape(step_count, TOK_DEV, D)
    grad_blocks = key_grad.reshape(step_count, TOK_DEV, KEY_WIDTH)

    def accumulate(total, pieces):
        rows_in, grads_in = pieces
        added = jnp.dot(rows_in.astype(jnp.float32).T, grads_in.astype(jnp.float32), preferred_element_type=jnp.float32)
        return total + added, None

    grad_key, ignored = lax.scan(accumulate, jnp.zeros((D, KEY_WIDTH), jnp.float32), (token_blocks, grad_blocks))

    def precondition(slot_index):
        left_part = jnp.dot(left_root[slot_index].astype(jnp.float32), slot_grads[slot_index].astype(jnp.float32), preferred_element_type=jnp.float32).astype(jnp.bfloat16)
        return jnp.dot(left_part.astype(jnp.float32), right_root[slot_index].astype(jnp.float32), preferred_element_type=jnp.float32).astype(jnp.bfloat16)

    blocks = lax.map(precondition, block_slot)
    update = jnp.transpose(blocks, (1, 0, 2))
    return grad_key, update
```

```python
import functools

import jax
import jax.numpy as jnp
from jax import lax
from jax.experimental import pallas as pl
from jax.experimental.pallas import tpu as pltpu
from jax.sharding import Mesh
from jax.sharding import PartitionSpec as P

AXES = ("rep", "shard_0", "shard_1", "shard_2", "shard_3")
SHARD = AXES[1:]
MESH = pl.DeviceIdType.MESH
F32 = jnp.float32
BF16 = jnp.bfloat16
NZ, NX, NY = 8, 4, 4
NSH = 128


def dot(a, b):
    return lax.dot_general(a, b, (((1,), (0,)), ((), ())), preferred_element_type=F32)


def dot_t(a, b):
    return lax.dot_general(a, b, (((0,), (0,)), ((), ())), preferred_element_type=F32)


def iota(shape, dim):
    return lax.broadcasted_iota(jnp.int32, shape, dim)


def drain(ref, sem):
    pltpu.make_async_copy(ref, ref, sem).wait()


def kernel(
    x_hbm, kg_hbm, left_hbm, grads_hbm, right_hbm, slot_ref,
    gk_out, up_out,
    xs, kgs, left_v, grads_v, right_v,
    t1, r1, s1, r2, s2, r3, fin,
    prod, recv, own, comp, comp_in, upd,
    x_sem, x_rsem, kg_sem, w_sem,
    send_core, send_key, send1, send2, send3, sem1, sem2, sem3, send_f, sem_f, loc_f,
    send_a, sem_a, send_c, sem_c, out_sem,
):
    e = lax.axis_index("rep")
    z = lax.axis_index("shard_0")
    l = lax.axis_index("shard_1")
    y = lax.axis_index("shard_2")
    c = lax.axis_index("shard_3")
    xp = e * 2 + l
    me = ((z * 2 + l) * 4 + y) * 2 + c
    partner = (e, z, l, y, 1 - c)

    def remote(src, dst, send_sem, recv_sem, device):
        pltpu.make_async_remote_copy(
            src_ref=src, dst_ref=dst, send_sem=send_sem, recv_sem=recv_sem,
            device_id=device, device_id_type=MESH,
        ).start()

    weights = ((left_hbm, left_v), (grads_hbm, grads_v), (right_hbm, right_v))
    for i, (src, dst) in enumerate(weights):
        pltpu.make_async_copy(src, dst, w_sem.at[i]).start()
    my_rows = pl.ds(pl.multiple_of(c * 256, 256), 256)

    def key_half(which):
        return kg_hbm.at[:, pl.ds(pl.multiple_of(which * 512, 512), 512)]

    remote(key_half(1 - c), kgs.at[my_rows, :], send_key, kg_sem.at[1], partner)
    pltpu.make_async_copy(key_half(c), kgs.at[my_rows, :], kg_sem.at[0]).start()

    def z_of(k):
        return lax.rem(z + 1 + k, NZ)

    def x_piece(k):
        return x_hbm.at[:, pl.ds(pl.multiple_of(z_of(k) * 512, 512), 512)]

    def fetch(k, carry):
        remote(x_piece(k), xs.at[k, my_rows, :], send_core, x_rsem.at[k], partner)
        pltpu.make_async_copy(x_piece(k), xs.at[k, my_rows, :], x_sem.at[k]).start()
        return carry

    lax.fori_loop(0, NZ, fetch, 0)

    slot_row = slot_ref[...]
    eye = iota((256, 256), 0) == iota((256, 256), 1)
    row_b = jnp.broadcast_to(slot_row, (256, 256))
    slot_col = jnp.sum(jnp.where(eye, row_b, 0), axis=1, keepdims=True)
    col_b = jnp.broadcast_to(slot_col, (256, 256))
    same = (row_b >> 2) == (col_b >> 2)
    less_r = col_b < row_b
    less_c = row_b < col_b
    g_row = jnp.sum(jnp.where(less_r, 1, 0), axis=0, keepdims=True)
    k_row = jnp.sum(jnp.where(less_r & same, 1, 0), axis=0, keepdims=True)
    g_col = jnp.sum(jnp.where(less_c, 1, 0), axis=1, keepdims=True)
    k_col = jnp.sum(jnp.where(less_c & same, 1, 0), axis=1, keepdims=True)
    mine_row = (g_row & 1) == e
    mine_col = (g_col & 1) == e

    for i, (src, dst) in enumerate(weights):
        pltpu.make_async_copy(src, dst, w_sem.at[i]).wait()
    parts = []
    for j in range(2):
        hit = mine_row & ((slot_row >> 2) == me) & ((k_row >> 1) == j)
        s = jnp.sum(jnp.where(hit, slot_row & 3, 0))
        half = dot(left_v[s], grads_v[s]).astype(BF16)
        parts.append(dot(half, right_v[s]).astype(BF16))

    out_row = iota((256, 256), 0)
    source = ((out_row >> 2) & 1) * 128 + (out_row >> 3) * 4 + (out_row & 3)
    perm = jnp.where(source == iota((256, 256), 1), 1.0, 0.0).astype(BF16)
    for q in range(4):
        stacked = jnp.concatenate([p[q * 128 : (q + 1) * 128] for p in parts], axis=0)
        moved = dot(perm, stacked).astype(BF16)
        prod[pl.ds(q * 32, 32)] = moved.reshape(32, 8, 512)

    def send_rows(i, carry):
        tz = lax.rem(z + lax.rem(i, 8), 8)
        tl = lax.rem(l + lax.rem(i // 8, 2), 2)
        ty = lax.rem(y + lax.rem(i // 16, 4), 4)
        tc = lax.rem(c + i // 64, 2)
        there = ((tz * 2 + tl) * 4 + ty) * 2 + tc
        remote(prod.at[there], recv.at[me], send_a, sem_a, (e, tz, tl, ty, tc))
        return carry

    lax.fori_loop(1, NSH, send_rows, 0)
    recv[me] = prod[me]

    drain(kgs.at[my_rows, :], kg_sem.at[0])
    drain(kgs.at[my_rows, :], kg_sem.at[1])

    def x_dev(p):
        return (p // 2, z, lax.rem(p, 2), y, c)

    def y_dev(p):
        return (e, z, l, p, c)

    def multiply(k, carry):
        drain(xs.at[k, my_rows, :], x_sem.at[k])
        drain(xs.at[k, my_rows, :], x_rsem.at[k])
        acc = dot_t(xs[k], kgs[...])
        for xl in range(2):
            for yy in range(NY):
                for xe in range(2):
                    base = (xl * 4 + yy) * 64
                    cols = slice(xe * 256, (xe + 1) * 256)
                    t1[k, 0, yy, xe * 2 + xl] = acc[base : base + 32, cols].astype(BF16)
                    t1[k, 1, xe * 2 + xl, yy] = acc[base + 32 : base + 64, cols].astype(BF16)
        for o in range(1, 4):
            to_y, to_x = lax.rem(y + o, 4), lax.rem(xp + o, 4)
            remote(t1.at[k, 0, to_y], r1.at[k, 0, o - 1], send1, sem1.at[k], y_dev(to_y))
            remote(t1.at[k, 1, to_x], r1.at[k, 1, o - 1], send1, sem1.at[k], x_dev(to_x))
        return carry

    lax.fori_loop(0, NZ, multiply, 0)

    def first_sum(k):
        drain(r1.at[k], sem1.at[k])
        for h, at in enumerate((y, xp)):
            total = t1[k, h, at].astype(F32)
            for o in range(3):
                total = total + r1[k, h, o].astype(F32)
            s1[k, h] = total.astype(BF16)
        for o in range(1, 4):
            to_y, to_x = lax.rem(y + o, 4), lax.rem(xp + o, 4)
            remote(s1.at[k, 0, to_x], r2.at[k, 0, o - 1], send2, sem2.at[k], x_dev(to_x))
            remote(s1.at[k, 1, to_y], r2.at[k, 1, o - 1], send2, sem2.at[k], y_dev(to_y))

    def second_total(k, h, at):
        total = s1[k, h, at].astype(F32)
        for o in range(3):
            total = total + r2[k, h, o].astype(F32)
        return total

    def second_sum(k):
        drain(r2.at[k], sem2.at[k])
        for h, at in enumerate((xp, y)):
            s2[k, h] = second_total(k, h, at).astype(BF16)
        remote(s2.at[k], r3.at[k], send3, sem3, (e, z_of(k), l, y, c))

    def sums(k, carry):
        first_sum(k)

        @pl.when(k > 0)
        def _():
            second_sum(k - 1)

        return carry

    lax.fori_loop(0, NZ, sums, 0)

    drain(recv.at[pl.ds(0, NSH - 1)], sem_a)
    pick = jnp.where(
        ((g_row >> 1) == iota((128, 256), 0)) & mine_row, 1.0, 0.0
    ).astype(BF16)
    place = jnp.where(
        ((g_col >> 1) == iota((256, 128), 1)) & jnp.logical_not(mine_col), 1.0, 0.0
    ).astype(BF16)
    first = jnp.where(mine_col, ((slot_col >> 2) * 2 + (k_col >> 1)) * 4, -8)
    other_rep = (1 - e, z, l, y, c)

    def compact(r, carry):
        chosen = jnp.where(iota((256, 1024), 1) == first + r, 1.0, 0.0).astype(BF16)
        rows = dot(chosen, recv[...].reshape(1024, 512)).astype(BF16)
        own[r] = rows
        comp[r] = dot(pick, rows).astype(BF16)
        remote(comp.at[r], comp_in.at[r], send_c, sem_c.at[r], other_rep)
        return carry

    lax.fori_loop(0, 4, compact, 0)

    drain(r2.at[NZ - 1], sem2.at[NZ - 1])
    drain(r3, sem3)
    for h, at in enumerate((xp, y)):
        total = second_total(NZ - 1, h, at)
        for k in range(NZ - 1):
            total = total + r3[k, h].astype(F32)
        fin[h] = total
    here = gk_out.at[:, pl.ds(pl.multiple_of((c * 2 + e) * 256, 256), 256)]
    pltpu.make_async_copy(fin.at[c], here, loc_f).start()
    remote(fin.at[c], here, send_f, sem_f, (1 - e, z, l, y, c))
    remote(fin.at[1 - c], here, send_f, sem_f, (e, z, l, y, 1 - c))
    remote(fin.at[1 - c], here, send_f, sem_f, (1 - e, z, l, y, 1 - c))

    def assemble(r, carry):
        drain(comp_in.at[r], sem_c.at[r])
        upd[r] = (dot(place, comp_in[r]) + own[r].astype(F32)).astype(BF16)
        pltpu.make_async_copy(upd.at[r], up_out.at[r], out_sem).start()
        return carry

    lax.fori_loop(0, 4, assemble, 0)
    drain(upd, out_sem)
    drain(fin.at[0], loc_f)
    drain(gk_out.at[:, pl.ds(0, 768)], sem_f)
    drain(gk_out.at[:, pl.ds(0, 768)], send_f)
    drain(kgs.at[my_rows, :], send_key)
    drain(xs.at[:, my_rows, :], send_core)
    drain(r1, send1)
    drain(r2, send2)
    drain(r3, send3)
    drain(recv.at[pl.ds(0, NSH - 1)], send_a)
    drain(comp, send_c)


def shards(tokens_x, key_grad, left_root, slot_grads, right_root, block_slot):
    any_space = pl.BlockSpec(memory_space=pl.ANY)
    vmem = pltpu.VMEM
    dma = pltpu.SemaphoreType.DMA
    return pl.pallas_call(
        kernel,
        out_shape=(
            jax.ShapeDtypeStruct((32, 1024), F32),
            jax.ShapeDtypeStruct((4, 256, 512), BF16),
        ),
        in_specs=[any_space] * 5 + [pl.BlockSpec(memory_space=pltpu.VMEM)],
        out_specs=(any_space, any_space),
        scratch_shapes=[
            vmem((8, 512, 512), BF16),
            vmem((512, 512), BF16),
            vmem((4, 512, 512), BF16),
            vmem((4, 512, 512), BF16),
            vmem((4, 512, 512), BF16),
            vmem((8, 2, 4, 4, 32, 256), BF16),
            vmem((8, 2, 3, 4, 32, 256), BF16),
            vmem((8, 2, 4, 32, 256), BF16),
            vmem((8, 2, 3, 32, 256), BF16),
            vmem((7, 2, 32, 256), BF16),
            vmem((7, 2, 32, 256), BF16),
            vmem((2, 32, 256), F32),
            vmem((128, 8, 512), BF16),
            vmem((128, 8, 512), BF16),
            vmem((4, 256, 512), BF16),
            vmem((4, 128, 512), BF16),
            vmem((4, 128, 512), BF16),
            vmem((4, 256, 512), BF16),
            dma((8,)), dma((8,)), dma((2,)), dma((3,)),
            dma, dma, dma, dma, dma, dma((8,)), dma((8,)), dma, dma, dma, dma,
            dma, dma, dma, dma((4,)), dma,
        ],
        compiler_params=pltpu.CompilerParams(has_side_effects=True),
        cost_estimate=pl.CostEstimate(
            flops=6 * 10**9, bytes_accessed=10 * 2**20, transcendentals=0
        ),
    )(tokens_x, key_grad, left_root, slot_grads, right_root, block_slot.reshape(1, 256))


def solution(mesh):
    finer = Mesh(mesh.devices.reshape(mesh.shape["rep"], 8, 2, 4, 2), AXES)
    in_specs = (
        P(AXES, None),
        P(AXES, None),
        P(SHARD, None, None),
        P(SHARD, None, None),
        P(SHARD, None, None),
        P(),
    )
    out_specs = (P(SHARD, None), P(SHARD, None, None))
    return jax.shard_map(
        shards, mesh=finer, in_specs=in_specs, out_specs=out_specs, check_vma=False
    )
```

```python
import functools

import jax
import jax.numpy as jnp
from jax import lax
from jax.experimental import pallas as pl
from jax.experimental.pallas import tpu as pltpu
from jax.sharding import Mesh
from jax.sharding import PartitionSpec as P

AXES = ("rep", "shard_0", "shard_1", "shard_2", "shard_3")
SHARD = AXES[1:]
MESH = pl.DeviceIdType.MESH
F32 = jnp.float32
BF16 = jnp.bfloat16
NZ, NX, NY = 8, 4, 4
NSH = 128
LAGS = (2, 4, 6)
COMPACT = 7


def dot(a, b):
    return lax.dot_general(a, b, (((1,), (0,)), ((), ())), preferred_element_type=F32)


def dot_t(a, b):
    return lax.dot_general(a, b, (((0,), (0,)), ((), ())), preferred_element_type=F32)


def iota(shape, dim):
    return lax.broadcasted_iota(jnp.int32, shape, dim)


def drain(ref, sem):
    pltpu.make_async_copy(ref, ref, sem).wait()


def kernel(
    x_hbm, kg_hbm, left_hbm, grads_hbm, right_hbm, slot_ref,
    gk_out, up_out,
    xs, kgs, left_v, grads_v, right_v,
    t1, rel, cmb, r1, s1, r2, s2, r3, fin,
    prod, recv, own, comp, comp_in, upd,
    x_sem, x_rsem, kg_sem, w_sem,
    send_core, send_key, send_rel, send_dir, send_cmb, send2, send3, sem_rel, sem1, sem2, sem3, send_f, sem_f, loc_f,
    send_a, sem_a, send_c, sem_c, out_sem,
):
    e = lax.axis_index("rep")
    z = lax.axis_index("shard_0")
    l = lax.axis_index("shard_1")
    y = lax.axis_index("shard_2")
    c = lax.axis_index("shard_3")
    xp = e * 2 + l
    me = ((z * 2 + l) * 4 + y) * 2 + c
    partner = (e, z, l, y, 1 - c)

    def remote(src, dst, send_sem, recv_sem, device):
        pltpu.make_async_remote_copy(
            src_ref=src, dst_ref=dst, send_sem=send_sem, recv_sem=recv_sem,
            device_id=device, device_id_type=MESH,
        ).start()

    barrier = pltpu.get_barrier_semaphore()

    def peer(k, m):
        tz = lax.rem(z + k + m, NZ)
        return (
            e, tz, lax.rem(l + m % 2, 2), lax.rem(y + m // 2 % 4, 4), lax.rem(c + m // 8, 2)
        )

    def greet(there):
        pl.semaphore_signal(barrier, inc=1, device_id=there, device_id_type=MESH)

    def greet_all(k, carry):
        @pl.when(k > 0)
        def _():
            greet(peer(k, 0))

        for m in range(1, 16):
            greet(peer(k, m))
        return carry

    for there in ((1 - e, z, l, y, c), (1 - e, z, l, y, 1 - c), (1 - e, z, 1 - l, y, c)):
        greet(there)
    lax.fori_loop(0, NZ, greet_all, 0)

    weights = ((left_hbm, left_v), (grads_hbm, grads_v), (right_hbm, right_v))
    for i, (src, dst) in enumerate(weights):
        pltpu.make_async_copy(src, dst, w_sem.at[i]).start()
    my_rows = pl.ds(pl.multiple_of(c * 256, 256), 256)

    def key_half(which):
        return kg_hbm.at[:, pl.ds(pl.multiple_of(which * 512, 512), 512)]

    pltpu.make_async_copy(key_half(c), kgs.at[my_rows, :], kg_sem.at[0]).start()

    def z_of(k):
        return lax.rem(z + 1 + k, NZ)

    def x_piece(k):
        return x_hbm.at[:, pl.ds(pl.multiple_of(z_of(k) * 512, 512), 512)]

    def fetch(k, carry):
        pltpu.make_async_copy(x_piece(k), xs.at[k, my_rows, :], x_sem.at[k]).start()
        return carry

    lax.fori_loop(0, NZ, fetch, 0)

    def swap(k, carry):
        remote(x_piece(k), xs.at[k, my_rows, :], send_core, x_rsem.at[k], partner)
        return carry

    slot_row = slot_ref[...]
    eye = iota((256, 256), 0) == iota((256, 256), 1)
    row_b = jnp.broadcast_to(slot_row, (256, 256))
    slot_col = jnp.sum(jnp.where(eye, row_b, 0), axis=1, keepdims=True)
    col_b = jnp.broadcast_to(slot_col, (256, 256))
    same = (row_b >> 2) == (col_b >> 2)
    less_r = col_b < row_b
    less_c = row_b < col_b
    g_row = jnp.sum(jnp.where(less_r, 1, 0), axis=0, keepdims=True)
    k_row = jnp.sum(jnp.where(less_r & same, 1, 0), axis=0, keepdims=True)
    g_col = jnp.sum(jnp.where(less_c, 1, 0), axis=1, keepdims=True)
    k_col = jnp.sum(jnp.where(less_c & same, 1, 0), axis=1, keepdims=True)
    mine_row = (g_row & 1) == e
    mine_col = (g_col & 1) == e

    for i, (src, dst) in enumerate(weights):
        pltpu.make_async_copy(src, dst, w_sem.at[i]).wait()
    parts = []
    for j in range(2):
        if j == 1:
            pl.semaphore_wait(barrier, NSH + 2)
            remote(key_half(1 - c), kgs.at[my_rows, :], send_key, kg_sem.at[1], partner)
            lax.fori_loop(0, NZ, swap, 0)
        hit = mine_row & ((slot_row >> 2) == me) & ((k_row >> 1) == j)
        s = jnp.sum(jnp.where(hit, slot_row & 3, 0))
        half = dot(left_v[s], grads_v[s]).astype(BF16)
        parts.append(dot(half, right_v[s]).astype(BF16))

    out_row = iota((256, 256), 0)
    source = ((out_row >> 2) & 1) * 128 + (out_row >> 3) * 4 + (out_row & 3)
    perm = jnp.where(source == iota((256, 256), 1), 1.0, 0.0).astype(BF16)
    for q in range(4):
        stacked = jnp.concatenate([p[q * 128 : (q + 1) * 128] for p in parts], axis=0)
        moved = dot(perm, stacked).astype(BF16)
        prod[pl.ds(q * 32, 32)] = moved.reshape(32, 8, 512)

    def y_first(k, h):
        return True if h == 0 else lax.rem(k, 4) == 0

    def pick2(cond, a, b):
        return a if cond is True else jnp.where(cond, a, b)

    def ring(along_y, p):
        return (
            pick2(along_y, e, p // 2),
            z,
            pick2(along_y, l, lax.rem(p, 2)),
            pick2(along_y, p, y),
            c,
        )

    def other(along_y):
        return False if along_y is True else jnp.logical_not(along_y)

    def pos(along_y):
        if along_y is False:
            return xp
        return pick2(along_y, y, xp)

    def ring_of(along_y, p):
        if along_y is False:
            return (p // 2, z, lax.rem(p, 2), y, c)
        return ring(along_y, p)

    def step_to(p, o):
        return lax.rem(p + o, 4)

    lower, upper = pl.ds(0, 2), pl.ds(2, 2)

    def send_rows(k, m):
        device = peer(k, m)
        _, tz, tl, ty, tc = device
        there = ((tz * 2 + tl) * 4 + ty) * 2 + tc
        remote(prod.at[there], recv.at[me], send_a, sem_a, device)

    def send_all(k, carry):
        @pl.when(k > 0)
        def _():
            send_rows(k, 0)

        for m in range(1, 16):
            send_rows(k, m)
        return carry

    lax.fori_loop(0, NZ, send_all, 0)
    recv[me] = prod[me]

    drain(kgs.at[my_rows, :], kg_sem.at[0])
    drain(kgs.at[my_rows, :], kg_sem.at[1])

    def multiply(k):
        drain(xs.at[k, my_rows, :], x_sem.at[k])
        drain(xs.at[k, my_rows, :], x_rsem.at[k])
        acc = dot_t(xs[k], kgs[...])
        for h in range(2):
            along_y = y_first(k, h)
            for xl in range(2):
                for yy in range(NY):
                    for xe in range(2):
                        base = (xl * 4 + yy) * 64 + h * 32
                        cols = slice(xe * 256, (xe + 1) * 256)
                        xx = xe * 2 + xl
                        piece = acc[base : base + 32, cols].astype(BF16)
                        t1[k, h, pick2(along_y, yy, xx), pick2(along_y, xx, yy)] = piece
        for h in range(2):
            along_y = y_first(k, h)
            p = pos(along_y)
            nxt, far, prv = step_to(p, 1), step_to(p, 2), step_to(p, 3)
            to_n, to_p = ring_of(along_y, nxt), ring_of(along_y, prv)
            remote(t1.at[k, h, far, lower], rel.at[k, h, 0], send_rel, sem_rel.at[k], to_n)
            remote(t1.at[k, h, far, upper], rel.at[k, h, 1], send_rel, sem_rel.at[k], to_p)
            remote(t1.at[k, h, nxt, upper], r1.at[k, h, 0, upper], send_dir, sem1.at[k], to_n)
            remote(t1.at[k, h, prv, lower], r1.at[k, h, 1, lower], send_dir, sem1.at[k], to_p)

    def relay(k):
        drain(rel.at[k], sem_rel.at[k])
        for h in range(2):
            along_y = y_first(k, h)
            p = pos(along_y)
            nxt, prv = step_to(p, 1), step_to(p, 3)
            half = t1[k, h, nxt, 0:2].astype(F32) + rel[k, h, 0].astype(F32)
            cmb[k, h, 0] = half.astype(BF16)
            remote(cmb.at[k, h, 0], r1.at[k, h, 0, lower], send_cmb, sem1.at[k], ring_of(along_y, nxt))
            half = t1[k, h, prv, 2:4].astype(F32) + rel[k, h, 1].astype(F32)
            cmb[k, h, 1] = half.astype(BF16)
            remote(cmb.at[k, h, 1], r1.at[k, h, 1, upper], send_cmb, sem1.at[k], ring_of(along_y, prv))

    def first_sum(k):
        drain(r1.at[k], sem1.at[k])
        for h in range(2):
            along_y = y_first(k, h)
            total = t1[k, h, pos(along_y)].astype(F32)
            s1[k, h] = (total + r1[k, h, 0].astype(F32) + r1[k, h, 1].astype(F32)).astype(BF16)
        for h in range(2):
            along_y = other(y_first(k, h))
            p = pos(along_y)
            for o in (2, 1, 3):
                to = step_to(p, o)
                remote(s1.at[k, h, to], r2.at[k, h, o - 1], send2, sem2.at[k], ring_of(along_y, to))

    def second_total(k, h):
        total = s1[k, h, pos(other(y_first(k, h)))].astype(F32)
        for o in range(3):
            total = total + r2[k, h, o].astype(F32)
        return total

    def second_sum(k):
        drain(r2.at[k], sem2.at[k])
        for h in range(2):
            s2[k, h] = second_total(k, h).astype(BF16)
        remote(s2.at[k], r3.at[k], send3, sem3, (e, z_of(k), l, y, c))

    pick = jnp.where(
        ((g_row >> 1) == iota((128, 256), 0)) & mine_row, 1.0, 0.0
    ).astype(BF16)
    place = jnp.where(
        ((g_col >> 1) == iota((256, 128), 1)) & jnp.logical_not(mine_col), 1.0, 0.0
    ).astype(BF16)
    first = jnp.where(mine_col, ((slot_col >> 2) * 2 + (k_col >> 1)) * 4, -8)
    other_rep = (1 - e, z, l, y, c)

    def compact(r):
        chosen = jnp.where(iota((256, 1024), 1) == first + r, 1.0, 0.0).astype(BF16)
        rows = dot(chosen, recv[...].reshape(1024, 512)).astype(BF16)
        own[r] = rows
        comp[r] = dot(pick, rows).astype(BF16)
        remote(comp.at[r], comp_in.at[r], send_c, sem_c.at[r], other_rep)

    def within(i, lag, count):
        return (i >= lag) & (i < lag + count)

    def steps(i, carry):
        @pl.when(i < NZ)
        def _():
            multiply(i)

        @pl.when(within(i, LAGS[0], NZ))
        def _():
            relay(i - LAGS[0])

        @pl.when(within(i, LAGS[1], NZ))
        def _():
            first_sum(i - LAGS[1])

        @pl.when(within(i, LAGS[2], NZ - 1))
        def _():
            second_sum(i - LAGS[2])

        @pl.when(i == COMPACT)
        def _():
            drain(recv.at[pl.ds(0, NSH - 1)], sem_a)

        @pl.when(within(i, COMPACT, 4))
        def _():
            compact(i - COMPACT)

        return carry

    lax.fori_loop(0, max(NZ + LAGS[1], NZ - 1 + LAGS[2]), steps, 0)

    def assemble(r, carry):
        drain(comp_in.at[r], sem_c.at[r])
        upd[r] = (dot(place, comp_in[r]) + own[r].astype(F32)).astype(BF16)
        pltpu.make_async_copy(upd.at[r], up_out.at[r], out_sem).start()
        return carry

    lax.fori_loop(0, 4, assemble, 0)

    drain(r2.at[NZ - 1], sem2.at[NZ - 1])
    drain(r3, sem3)
    for h in range(2):
        total = second_total(NZ - 1, h)
        for k in range(NZ - 1):
            total = total + r3[k, h].astype(F32)
        fin[h] = total
    here = gk_out.at[:, pl.ds(pl.multiple_of((c * 2 + e) * 256, 256), 256)]
    pltpu.make_async_copy(fin.at[c], here, loc_f).start()
    remote(fin.at[c], here, send_f, sem_f, (1 - e, z, l, y, c))
    remote(fin.at[1 - c], here, send_f, sem_f, (e, z, l, y, 1 - c))
    remote(fin.at[1 - c], here, send_f, sem_f, (1 - e, z, l, y, 1 - c))

    drain(upd, out_sem)
    drain(fin.at[0], loc_f)
    drain(gk_out.at[:, pl.ds(0, 768)], sem_f)
    drain(gk_out.at[:, pl.ds(0, 768)], send_f)
    drain(kgs.at[my_rows, :], send_key)
    drain(xs.at[:, my_rows, :], send_core)
    drain(rel, send_rel)
    drain(rel, send_dir)
    drain(cmb, send_cmb)
    drain(r2, send2)
    drain(r3, send3)
    drain(recv.at[pl.ds(0, NSH - 1)], send_a)
    drain(comp, send_c)


def shards(tokens_x, key_grad, left_root, slot_grads, right_root, block_slot):
    any_space = pl.BlockSpec(memory_space=pl.ANY)
    vmem = pltpu.VMEM
    dma = pltpu.SemaphoreType.DMA
    return pl.pallas_call(
        kernel,
        out_shape=(
            jax.ShapeDtypeStruct((32, 1024), F32),
            jax.ShapeDtypeStruct((4, 256, 512), BF16),
        ),
        in_specs=[any_space] * 5 + [pl.BlockSpec(memory_space=pltpu.VMEM)],
        out_specs=(any_space, any_space),
        scratch_shapes=[
            vmem((8, 512, 512), BF16),
            vmem((512, 512), BF16),
            vmem((4, 512, 512), BF16),
            vmem((4, 512, 512), BF16),
            vmem((4, 512, 512), BF16),
            vmem((8, 2, 4, 4, 32, 256), BF16),
            vmem((8, 2, 2, 2, 32, 256), BF16),
            vmem((8, 2, 2, 2, 32, 256), BF16),
            vmem((8, 2, 2, 4, 32, 256), BF16),
            vmem((8, 2, 4, 32, 256), BF16),
            vmem((8, 2, 3, 32, 256), BF16),
            vmem((7, 2, 32, 256), BF16),
            vmem((7, 2, 32, 256), BF16),
            vmem((2, 32, 256), F32),
            vmem((128, 8, 512), BF16),
            vmem((128, 8, 512), BF16),
            vmem((4, 256, 512), BF16),
            vmem((4, 128, 512), BF16),
            vmem((4, 128, 512), BF16),
            vmem((4, 256, 512), BF16),
            dma((8,)), dma((8,)), dma((2,)), dma((3,)),
            dma, dma, dma, dma, dma, dma, dma, dma((8,)), dma((8,)), dma((8,)), dma, dma, dma, dma,
            dma, dma, dma, dma((4,)), dma,
        ],
        compiler_params=pltpu.CompilerParams(has_side_effects=True, collective_id=0),
        cost_estimate=pl.CostEstimate(
            flops=6 * 10**9, bytes_accessed=10 * 2**20, transcendentals=0
        ),
    )(tokens_x, key_grad, left_root, slot_grads, right_root, block_slot.reshape(1, 256))


def solution(mesh):
    finer = Mesh(mesh.devices.reshape(mesh.shape["rep"], 8, 2, 4, 2), AXES)
    in_specs = (
        P(AXES, None),
        P(AXES, None),
        P(SHARD, None, None),
        P(SHARD, None, None),
        P(SHARD, None, None),
        P(),
    )
    out_specs = (P(SHARD, None), P(SHARD, None, None))
    return jax.shard_map(
        shards, mesh=finer, in_specs=in_specs, out_specs=out_specs, check_vma=False
    )
```

```python
import functools

import jax
import jax.numpy as jnp
from jax import lax
from jax.experimental import pallas as pl
from jax.experimental.pallas import tpu as pltpu
from jax.sharding import Mesh
from jax.sharding import PartitionSpec as P

AXES = ("rep", "shard_0", "shard_1", "shard_2", "shard_3")
SHARD = AXES[1:]
MESH = pl.DeviceIdType.MESH
F32 = jnp.float32
BF16 = jnp.bfloat16
NZ, NX, NY = 8, 4, 4
NSH = 128
LAGS = (2, 4, 6)
COMPACT = 7


def dot(a, b):
    return lax.dot_general(a, b, (((1,), (0,)), ((), ())), preferred_element_type=F32)


def dot_t(a, b):
    return lax.dot_general(a, b, (((0,), (0,)), ((), ())), preferred_element_type=F32)


def iota(shape, dim):
    return lax.broadcasted_iota(jnp.int32, shape, dim)


def drain(ref, sem):
    pltpu.make_async_copy(ref, ref, sem).wait()


def kernel(
    x_hbm, kg_hbm, left_hbm, grads_hbm, right_hbm, slot_hbm,
    gk_out, up_out,
    slot_ref, xs, kgs, left_v, grads_v, right_v,
    t1, rel, cmb, r1, s1, r2, s2, r3, fin,
    prod, recv, own, comp, comp_in, upd,
    x_sem, x_rsem, kg_sem, w_sem,
    send_core, send_key, send_rel, send_dir, send_cmb, send2, send3, sem_rel, sem1, sem2, sem3, send_f, sem_f, loc_f,
    send_a, sem_a, send_c, sem_c, out_sem,
):
    e = lax.axis_index("rep")
    z = lax.axis_index("shard_0")
    l = lax.axis_index("shard_1")
    y = lax.axis_index("shard_2")
    c = lax.axis_index("shard_3")
    xp = e * 2 + l
    me = ((z * 2 + l) * 4 + y) * 2 + c
    partner = (e, z, l, y, 1 - c)

    def remote(src, dst, send_sem, recv_sem, device):
        pltpu.make_async_remote_copy(
            src_ref=src, dst_ref=dst, send_sem=send_sem, recv_sem=recv_sem,
            device_id=device, device_id_type=MESH,
        ).start()

    slots = pltpu.make_async_copy(slot_hbm, slot_ref, w_sem.at[3])
    slots.start()
    weights = ((left_hbm, left_v), (grads_hbm, grads_v), (right_hbm, right_v))
    for i, (src, dst) in enumerate(weights):
        pltpu.make_async_copy(src, dst, w_sem.at[i]).start()

    barrier = pltpu.get_barrier_semaphore()

    def peer(k, m):
        tz = lax.rem(z + k + m, NZ)
        return (
            e, tz, lax.rem(l + m % 2, 2), lax.rem(y + m // 2 % 4, 4), lax.rem(c + m // 8, 2)
        )

    def greet(there):
        pl.semaphore_signal(barrier, inc=1, device_id=there, device_id_type=MESH)

    def greet_all(k, carry):
        @pl.when(k > 0)
        def _():
            greet(peer(k, 0))

        for m in range(1, 16):
            greet(peer(k, m))
        return carry

    for there in ((1 - e, z, l, y, c), (1 - e, z, l, y, 1 - c), (1 - e, z, 1 - l, y, c)):
        greet(there)
    lax.fori_loop(0, NZ, greet_all, 0)

    my_rows = pl.ds(pl.multiple_of(c * 256, 256), 256)

    def key_half(which):
        return kg_hbm.at[:, pl.ds(pl.multiple_of(which * 512, 512), 512)]

    pltpu.make_async_copy(key_half(c), kgs.at[my_rows, :], kg_sem.at[0]).start()

    def z_of(k):
        return lax.rem(z + 1 + k, NZ)

    def x_piece(k):
        return x_hbm.at[:, pl.ds(pl.multiple_of(z_of(k) * 512, 512), 512)]

    def fetch(k, carry):
        pltpu.make_async_copy(x_piece(k), xs.at[k, my_rows, :], x_sem.at[k]).start()
        return carry

    lax.fori_loop(0, NZ, fetch, 0)

    def swap(k, carry):
        remote(x_piece(k), xs.at[k, my_rows, :], send_core, x_rsem.at[k], partner)
        return carry

    slots.wait()
    slot_row = slot_ref[...]
    eye = iota((256, 256), 0) == iota((256, 256), 1)
    row_b = jnp.broadcast_to(slot_row, (256, 256))
    slot_col = jnp.sum(jnp.where(eye, row_b, 0), axis=1, keepdims=True)
    col_b = jnp.broadcast_to(slot_col, (256, 256))
    same = (row_b >> 2) == (col_b >> 2)
    less_r = col_b < row_b
    less_c = row_b < col_b
    g_row = jnp.sum(jnp.where(less_r, 1, 0), axis=0, keepdims=True)
    k_row = jnp.sum(jnp.where(less_r & same, 1, 0), axis=0, keepdims=True)
    g_col = jnp.sum(jnp.where(less_c, 1, 0), axis=1, keepdims=True)
    k_col = jnp.sum(jnp.where(less_c & same, 1, 0), axis=1, keepdims=True)
    mine_row = (g_row & 1) == e
    mine_col = (g_col & 1) == e

    for i in range(2):
        drain(left_v, w_sem.at[i])
    parts = []
    for j in range(2):
        if j == 1:
            pl.semaphore_wait(barrier, NSH + 2)
            remote(key_half(1 - c), kgs.at[my_rows, :], send_key, kg_sem.at[1], partner)
            lax.fori_loop(0, NZ, swap, 0)
        hit = mine_row & ((slot_row >> 2) == me) & ((k_row >> 1) == j)
        s = jnp.sum(jnp.where(hit, slot_row & 3, 0))
        half = dot(left_v[s], grads_v[s]).astype(BF16)
        if j == 0:
            drain(right_v, w_sem.at[2])
        parts.append(dot(half, right_v[s]).astype(BF16))

    out_row = iota((256, 256), 0)
    source = ((out_row >> 2) & 1) * 128 + (out_row >> 3) * 4 + (out_row & 3)
    perm = jnp.where(source == iota((256, 256), 1), 1.0, 0.0).astype(BF16)
    for q in range(4):
        stacked = jnp.concatenate([p[q * 128 : (q + 1) * 128] for p in parts], axis=0)
        moved = dot(perm, stacked).astype(BF16)
        prod[pl.ds(q * 32, 32)] = moved.reshape(32, 8, 512)

    def y_first(k, h):
        return (k >= 0) if h == 0 else (k < 0)

    def pick2(cond, a, b):
        return a if cond is True else jnp.where(cond, a, b)

    def ring(along_y, p):
        return (
            pick2(along_y, e, p // 2),
            z,
            pick2(along_y, l, lax.rem(p, 2)),
            pick2(along_y, p, y),
            c,
        )

    def other(along_y):
        return False if along_y is True else jnp.logical_not(along_y)

    def pos(along_y):
        if along_y is False:
            return xp
        return pick2(along_y, y, xp)

    def ring_of(along_y, p):
        if along_y is False:
            return (p // 2, z, lax.rem(p, 2), y, c)
        return ring(along_y, p)

    def step_to(p, o):
        return lax.rem(p + o, 4)

    lower, upper = pl.ds(0, 2), pl.ds(2, 2)

    def send_rows(k, m):
        device = peer(k, m)
        _, tz, tl, ty, tc = device
        there = ((tz * 2 + tl) * 4 + ty) * 2 + tc
        remote(prod.at[there], recv.at[me], send_a, sem_a, device)

    def send_all(k, carry):
        @pl.when(k > 0)
        def _():
            send_rows(k, 0)

        for m in range(1, 16):
            send_rows(k, m)
        return carry

    lax.fori_loop(0, NZ, send_all, 0)
    recv[me] = prod[me]

    drain(kgs.at[my_rows, :], kg_sem.at[0])
    drain(kgs.at[my_rows, :], kg_sem.at[1])

    def multiply(k):
        drain(xs.at[k, my_rows, :], x_sem.at[k])
        drain(xs.at[k, my_rows, :], x_rsem.at[k])
        acc = dot_t(xs[k], kgs[...])
        for h in range(2):
            along_y = y_first(k, h)
            for xl in range(2):
                for yy in range(NY):
                    for xe in range(2):
                        base = (xl * 4 + yy) * 64 + h * 32
                        cols = slice(xe * 256, (xe + 1) * 256)
                        xx = xe * 2 + xl
                        piece = acc[base : base + 32, cols].astype(BF16)
                        t1[k, h, pick2(along_y, yy, xx), pick2(along_y, xx, yy)] = piece
        for h in range(2):
            along_y = y_first(k, h)
            p = pos(along_y)
            nxt, far, prv = step_to(p, 1), step_to(p, 2), step_to(p, 3)
            to_n, to_p = ring_of(along_y, nxt), ring_of(along_y, prv)
            remote(t1.at[k, h, far, lower], rel.at[k, h, 0], send_rel, sem_rel.at[k], to_n)
            remote(t1.at[k, h, far, upper], rel.at[k, h, 1], send_rel, sem_rel.at[k], to_p)
            remote(t1.at[k, h, nxt, upper], r1.at[k, h, 0, upper], send_dir, sem1.at[k], to_n)
            remote(t1.at[k, h, prv, lower], r1.at[k, h, 1, lower], send_dir, sem1.at[k], to_p)

    def relay(k):
        drain(rel.at[k], sem_rel.at[k])
        for h in range(2):
            along_y = y_first(k, h)
            p = pos(along_y)
            nxt, prv = step_to(p, 1), step_to(p, 3)
            half = t1[k, h, nxt, 0:2].astype(F32) + rel[k, h, 0].astype(F32)
            cmb[k, h, 0] = half.astype(BF16)
            remote(cmb.at[k, h, 0], r1.at[k, h, 0, lower], send_cmb, sem1.at[k], ring_of(along_y, nxt))
            half = t1[k, h, prv, 2:4].astype(F32) + rel[k, h, 1].astype(F32)
            cmb[k, h, 1] = half.astype(BF16)
            remote(cmb.at[k, h, 1], r1.at[k, h, 1, upper], send_cmb, sem1.at[k], ring_of(along_y, prv))

    def first_sum(k):
        drain(r1.at[k], sem1.at[k])
        for h in range(2):
            along_y = y_first(k, h)
            total = t1[k, h, pos(along_y)].astype(F32)
            s1[k, h] = (total + r1[k, h, 0].astype(F32) + r1[k, h, 1].astype(F32)).astype(BF16)
        for h in range(2):
            along_y = other(y_first(k, h))
            p = pos(along_y)
            for o in (2, 1, 3):
                to = step_to(p, o)
                remote(s1.at[k, h, to], r2.at[k, h, o - 1], send2, sem2.at[k], ring_of(along_y, to))

    def second_total(k, h):
        total = s1[k, h, pos(other(y_first(k, h)))].astype(F32)
        for o in range(3):
            total = total + r2[k, h, o].astype(F32)
        return total

    def second_sum(k):
        drain(r2.at[k], sem2.at[k])
        for h in range(2):
            s2[k, h] = second_total(k, h).astype(BF16)
        remote(s2.at[k], r3.at[k], send3, sem3, (e, z_of(k), l, y, c))

    pick = jnp.where(
        ((g_row >> 1) == iota((128, 256), 0)) & mine_row, 1.0, 0.0
    ).astype(BF16)
    place = jnp.where(
        ((g_col >> 1) == iota((256, 128), 1)) & jnp.logical_not(mine_col), 1.0, 0.0
    ).astype(BF16)
    first = jnp.where(mine_col, ((slot_col >> 2) * 2 + (k_col >> 1)) * 4, -8)
    other_rep = (1 - e, z, l, y, c)

    def compact(r):
        chosen = jnp.where(iota((256, 1024), 1) == first + r, 1.0, 0.0).astype(BF16)
        rows = dot(chosen, recv[...].reshape(1024, 512)).astype(BF16)
        own[r] = rows
        comp[r] = dot(pick, rows).astype(BF16)
        remote(comp.at[r], comp_in.at[r], send_c, sem_c.at[r], other_rep)

    def within(i, lag, count):
        return (i >= lag) & (i < lag + count)

    def steps(i, carry):
        @pl.when(i < NZ)
        def _():
            multiply(i)

        @pl.when(within(i, LAGS[0], NZ))
        def _():
            relay(i - LAGS[0])

        @pl.when(within(i, LAGS[1], NZ))
        def _():
            first_sum(i - LAGS[1])

        @pl.when(within(i, LAGS[2], NZ - 1))
        def _():
            second_sum(i - LAGS[2])

        @pl.when(i == COMPACT)
        def _():
            drain(recv.at[pl.ds(0, NSH - 1)], sem_a)

        @pl.when(within(i, COMPACT, 4))
        def _():
            compact(i - COMPACT)

        return carry

    lax.fori_loop(0, max(NZ + LAGS[1], NZ - 1 + LAGS[2]), steps, 0)

    def assemble(r, carry):
        drain(comp_in.at[r], sem_c.at[r])
        up_out[r] = (dot(place, comp_in[r]) + own[r].astype(F32)).astype(BF16)
        return carry

    lax.fori_loop(0, 3, assemble, 0)

    drain(r2.at[NZ - 1], sem2.at[NZ - 1])
    drain(r3, sem3)
    for h in range(2):
        total = second_total(NZ - 1, h)
        for k in range(NZ - 1):
            total = total + r3[k, h].astype(F32)
        fin[h] = total
    here = gk_out.at[:, pl.ds(pl.multiple_of((c * 2 + e) * 256, 256), 256)]
    pltpu.make_async_copy(fin.at[c], here, loc_f).start()
    remote(fin.at[c], here, send_f, sem_f, (1 - e, z, l, y, c))
    remote(fin.at[1 - c], here, send_f, sem_f, (e, z, l, y, 1 - c))
    remote(fin.at[1 - c], here, send_f, sem_f, (1 - e, z, l, y, 1 - c))

    assemble(3, 0)
    drain(fin.at[0], loc_f)
    drain(gk_out.at[:, pl.ds(0, 768)], sem_f)
    drain(gk_out.at[:, pl.ds(0, 768)], send_f)
    drain(kgs.at[my_rows, :], send_key)
    drain(xs.at[:, my_rows, :], send_core)
    drain(rel, send_rel)
    drain(rel, send_dir)
    drain(cmb, send_cmb)
    drain(r2, send2)
    drain(r3, send3)
    drain(recv.at[pl.ds(0, NSH - 1)], send_a)
    drain(comp, send_c)


def shards(tokens_x, key_grad, left_root, slot_grads, right_root, block_slot):
    any_space = pl.BlockSpec(memory_space=pl.ANY)
    vmem = pltpu.VMEM
    dma = pltpu.SemaphoreType.DMA
    return pl.pallas_call(
        kernel,
        out_shape=(
            jax.ShapeDtypeStruct((32, 1024), F32),
            jax.ShapeDtypeStruct((4, 256, 512), BF16),
        ),
        in_specs=[any_space] * 6,
        out_specs=(pl.BlockSpec(memory_space=pltpu.VMEM), pl.BlockSpec(memory_space=pltpu.VMEM)),
        scratch_shapes=[
            vmem((1, 256), jnp.int32),
            vmem((8, 512, 512), BF16),
            vmem((512, 512), BF16),
            vmem((4, 512, 512), BF16),
            vmem((4, 512, 512), BF16),
            vmem((4, 512, 512), BF16),
            vmem((8, 2, 4, 4, 32, 256), BF16),
            vmem((8, 2, 2, 2, 32, 256), BF16),
            vmem((8, 2, 2, 2, 32, 256), BF16),
            vmem((8, 2, 2, 4, 32, 256), BF16),
            vmem((8, 2, 4, 32, 256), BF16),
            vmem((8, 2, 3, 32, 256), BF16),
            vmem((7, 2, 32, 256), BF16),
            vmem((7, 2, 32, 256), BF16),
            vmem((2, 32, 256), F32),
            vmem((128, 8, 512), BF16),
            vmem((128, 8, 512), BF16),
            vmem((4, 256, 512), BF16),
            vmem((4, 128, 512), BF16),
            vmem((4, 128, 512), BF16),
            vmem((4, 256, 512), BF16),
            dma((8,)), dma((8,)), dma((2,)), dma((4,)),
            dma, dma, dma, dma, dma, dma, dma, dma((8,)), dma((8,)), dma((8,)), dma, dma, dma, dma,
            dma, dma, dma, dma((4,)), dma,
        ],
        compiler_params=pltpu.CompilerParams(has_side_effects=True, collective_id=0, vmem_limit_bytes=51 * 2**20),
        cost_estimate=pl.CostEstimate(
            flops=6 * 10**9, bytes_accessed=10 * 2**20, transcendentals=0
        ),
    )(tokens_x, key_grad, left_root, slot_grads, right_root, block_slot.reshape(1, 256))


def solution(mesh):
    finer = Mesh(mesh.devices.reshape(mesh.shape["rep"], 8, 2, 4, 2), AXES)
    in_specs = (
        P(AXES, None),
        P(AXES, None),
        P(SHARD, None, None),
        P(SHARD, None, None),
        P(SHARD, None, None),
        P(),
    )
    out_specs = (P(SHARD, None), P(SHARD, None, None))
    return jax.shard_map(
        shards, mesh=finer, in_specs=in_specs, out_specs=out_specs, check_vma=False
    )
```

```python
import functools

import jax
import jax.numpy as jnp
from jax import lax
from jax.experimental import pallas as pl
from jax.experimental.pallas import tpu as pltpu
from jax.sharding import Mesh
from jax.sharding import PartitionSpec as P

AXES = ("rep", "shard_0", "shard_1", "shard_2", "shard_3")
SHARD = AXES[1:]
MESH = pl.DeviceIdType.MESH
F32 = jnp.float32
BF16 = jnp.bfloat16
NZ, NX, NY = 8, 4, 4
NSH = 128
LAGS = (2, 4, 6)
AHEAD = 2
COMPACT = 7


def dot(a, b):
    return lax.dot_general(a, b, (((1,), (0,)), ((), ())), preferred_element_type=F32)


def dot_t(a, b):
    return lax.dot_general(a, b, (((0,), (0,)), ((), ())), preferred_element_type=F32)


def iota(shape, dim):
    return lax.broadcasted_iota(jnp.int32, shape, dim)


def drain(ref, sem):
    pltpu.make_async_copy(ref, ref, sem).wait()


def kernel(
    x_hbm, kg_hbm, left_hbm, grads_hbm, right_hbm, slot_hbm,
    gk_out, up_out,
    slot_ref, xs, kgs, left_v, grads_v, right_v,
    t1, rel, cmb, r1, s1, r2, s2, r3, fin,
    prod, recv, own, comp, comp_in, upd,
    x_sem, x_rsem, kg_sem, w_sem,
    send_core, send_key, send_rel, send_dir, send_cmb, send2, send3, sem_rel, sem1, sem2, sem3, send_f, sem_f, loc_f,
    send_a, sem_a, send_c, sem_c, out_sem,
):
    e = lax.axis_index("rep")
    z = lax.axis_index("shard_0")
    l = lax.axis_index("shard_1")
    y = lax.axis_index("shard_2")
    c = lax.axis_index("shard_3")
    xp = e * 2 + l
    me = ((z * 2 + l) * 4 + y) * 2 + c
    partner = (e, z, l, y, 1 - c)

    def remote(src, dst, send_sem, recv_sem, device):
        pltpu.make_async_remote_copy(
            src_ref=src, dst_ref=dst, send_sem=send_sem, recv_sem=recv_sem,
            device_id=device, device_id_type=MESH,
        ).start()

    slots = pltpu.make_async_copy(slot_hbm, slot_ref, w_sem.at[3])
    slots.start()
    weights = ((left_hbm, left_v), (grads_hbm, grads_v), (right_hbm, right_v))
    for i, (src, dst) in enumerate(weights):
        pltpu.make_async_copy(src, dst, w_sem.at[i]).start()

    barrier = pltpu.get_barrier_semaphore()

    def peer(k, m):
        tz = lax.rem(z + k + m, NZ)
        return (
            e, tz, lax.rem(l + m % 2, 2), lax.rem(y + m // 2 % 4, 4), lax.rem(c + m // 8, 2)
        )

    def greet(there):
        pl.semaphore_signal(barrier, inc=1, device_id=there, device_id_type=MESH)

    def greet_all(k, carry):
        dz = 4 + (k + 1) // 2 * (1 - 2 * lax.rem(k, 2))
        tz = lax.rem(z + dz, NZ)
        for dy in (2, 1, 3, 0):
            for dl in (1, 0):
                for dc in (1, 0):
                    there = (e, tz, lax.rem(l + dl, 2), lax.rem(y + dy, 4), lax.rem(c + dc, 2))
                    if dy or dl or dc:
                        greet(there)
                    else:

                        @pl.when(k < NZ - 1)
                        def _():
                            greet(there)

        return carry

    for there in ((1 - e, z, l, y, c), (1 - e, z, l, y, 1 - c), (1 - e, z, 1 - l, y, c)):
        greet(there)
    lax.fori_loop(0, NZ, greet_all, 0)

    my_rows = pl.ds(pl.multiple_of(c * 256, 256), 256)

    def key_half(which):
        return kg_hbm.at[:, pl.ds(pl.multiple_of(which * 512, 512), 512)]

    pltpu.make_async_copy(key_half(c), kgs.at[my_rows, :], kg_sem.at[0]).start()

    def z_of(k):
        return lax.rem(z + 1 + k, NZ)

    def x_piece(k):
        return x_hbm.at[:, pl.ds(pl.multiple_of(z_of(k) * 512, 512), 512)]

    def fetch(k, carry):
        pltpu.make_async_copy(x_piece(k), xs.at[k, my_rows, :], x_sem.at[k]).start()
        return carry

    lax.fori_loop(0, NZ, fetch, 0)

    def swap(k, carry):
        remote(x_piece(k), xs.at[k, my_rows, :], send_core, x_rsem.at[k], partner)
        return carry

    slots.wait()
    slot_row = slot_ref[...]
    eye = iota((256, 256), 0) == iota((256, 256), 1)
    row_b = jnp.broadcast_to(slot_row, (256, 256))
    slot_col = jnp.sum(jnp.where(eye, row_b, 0), axis=1, keepdims=True)
    col_b = jnp.broadcast_to(slot_col, (256, 256))
    same = (row_b >> 2) == (col_b >> 2)
    less_r = col_b < row_b
    less_c = row_b < col_b
    g_row = jnp.sum(jnp.where(less_r, 1, 0), axis=0, keepdims=True)
    k_row = jnp.sum(jnp.where(less_r & same, 1, 0), axis=0, keepdims=True)
    g_col = jnp.sum(jnp.where(less_c, 1, 0), axis=1, keepdims=True)
    k_col = jnp.sum(jnp.where(less_c & same, 1, 0), axis=1, keepdims=True)
    mine_row = (g_row & 1) == e
    mine_col = (g_col & 1) == e

    for i in range(2):
        drain(left_v, w_sem.at[i])
    parts = []
    for j in range(2):
        hit = mine_row & ((slot_row >> 2) == me) & ((k_row >> 1) == j)
        s = jnp.sum(jnp.where(hit, slot_row & 3, 0))
        half = dot(left_v[s], grads_v[s]).astype(BF16)
        if j == 0:
            drain(right_v, w_sem.at[2])
        parts.append(dot(half, right_v[s]).astype(BF16))

    out_row = iota((256, 256), 0)
    source = ((out_row >> 2) & 1) * 128 + (out_row >> 3) * 4 + (out_row & 3)
    perm = jnp.where(source == iota((256, 256), 1), 1.0, 0.0).astype(BF16)
    for q in range(4):
        stacked = jnp.concatenate([p[q * 128 : (q + 1) * 128] for p in parts], axis=0)
        moved = dot(perm, stacked).astype(BF16)
        prod[pl.ds(q * 32, 32)] = moved.reshape(32, 8, 512)

    pl.semaphore_wait(barrier, NSH + 2)
    remote(key_half(1 - c), kgs.at[my_rows, :], send_key, kg_sem.at[1], partner)
    lax.fori_loop(0, NZ, swap, 0)

    def y_first(k, h):
        return (k >= 0) if h == 0 else (k < 0)

    def pick2(cond, a, b):
        return a if cond is True else jnp.where(cond, a, b)

    def ring(along_y, p):
        return (
            pick2(along_y, e, p // 2),
            z,
            pick2(along_y, l, lax.rem(p, 2)),
            pick2(along_y, p, y),
            c,
        )

    def other(along_y):
        return False if along_y is True else jnp.logical_not(along_y)

    def pos(along_y):
        if along_y is False:
            return xp
        return pick2(along_y, y, xp)

    def ring_of(along_y, p):
        if along_y is False:
            return (p // 2, z, lax.rem(p, 2), y, c)
        return ring(along_y, p)

    def step_to(p, o):
        return lax.rem(p + o, 4)

    lower, upper = pl.ds(0, 2), pl.ds(2, 2)

    def send_rows(k, m):
        device = peer(k, m)
        _, tz, tl, ty, tc = device
        there = ((tz * 2 + tl) * 4 + ty) * 2 + tc
        remote(prod.at[there], recv.at[me], send_a, sem_a, device)

    def send_all(k, carry):
        @pl.when(k > 0)
        def _():
            send_rows(k, 0)

        for m in range(1, 16):
            send_rows(k, m)
        return carry

    lax.fori_loop(0, NZ, send_all, 0)
    recv[me] = prod[me]

    drain(kgs.at[my_rows, :], kg_sem.at[0])
    drain(kgs.at[my_rows, :], kg_sem.at[1])

    def multiply(k, carry):
        drain(xs.at[k, my_rows, :], x_sem.at[k])
        drain(xs.at[k, my_rows, :], x_rsem.at[k])
        acc = dot_t(xs[k], kgs[...])
        for h in range(2):
            along_y = y_first(k, h)
            for xl in range(2):
                for yy in range(NY):
                    for xe in range(2):
                        base = (xl * 4 + yy) * 64 + h * 32
                        cols = slice(xe * 256, (xe + 1) * 256)
                        xx = xe * 2 + xl
                        piece = acc[base : base + 32, cols].astype(BF16)
                        t1[k, h, pick2(along_y, yy, xx), pick2(along_y, xx, yy)] = piece

        @pl.when(k < AHEAD)
        def _():
            send_direct(k)

        return carry

    def send_direct(k):
        for h in range(2):
            along_y = y_first(k, h)
            p = pos(along_y)
            nxt, far, prv = step_to(p, 1), step_to(p, 2), step_to(p, 3)
            to_n, to_p = ring_of(along_y, nxt), ring_of(along_y, prv)
            remote(t1.at[k, h, far, lower], rel.at[k, h, 0], send_rel, sem_rel.at[k], to_n)
            remote(t1.at[k, h, far, upper], rel.at[k, h, 1], send_rel, sem_rel.at[k], to_p)
            remote(t1.at[k, h, nxt, upper], r1.at[k, h, 0, upper], send_dir, sem1.at[k], to_n)
            remote(t1.at[k, h, prv, lower], r1.at[k, h, 1, lower], send_dir, sem1.at[k], to_p)

    def relay(k):
        drain(rel.at[k], sem_rel.at[k])
        for h in range(2):
            along_y = y_first(k, h)
            p = pos(along_y)
            nxt, prv = step_to(p, 1), step_to(p, 3)
            half = t1[k, h, nxt, 0:2].astype(F32) + rel[k, h, 0].astype(F32)
            cmb[k, h, 0] = half.astype(BF16)
            remote(cmb.at[k, h, 0], r1.at[k, h, 0, lower], send_cmb, sem1.at[k], ring_of(along_y, nxt))
            half = t1[k, h, prv, 2:4].astype(F32) + rel[k, h, 1].astype(F32)
            cmb[k, h, 1] = half.astype(BF16)
            remote(cmb.at[k, h, 1], r1.at[k, h, 1, upper], send_cmb, sem1.at[k], ring_of(along_y, prv))

    def first_sum(k):
        drain(r1.at[k], sem1.at[k])
        for h in range(2):
            along_y = y_first(k, h)
            total = t1[k, h, pos(along_y)].astype(F32)
            s1[k, h] = (total + r1[k, h, 0].astype(F32) + r1[k, h, 1].astype(F32)).astype(BF16)
        for h in range(2):
            along_y = other(y_first(k, h))
            p = pos(along_y)
            for o in (2, 1, 3):
                to = step_to(p, o)
                remote(s1.at[k, h, to], r2.at[k, h, o - 1], send2, sem2.at[k], ring_of(along_y, to))

    def second_total(k, h):
        total = s1[k, h, pos(other(y_first(k, h)))].astype(F32)
        for o in range(3):
            total = total + r2[k, h, o].astype(F32)
        return total

    def second_sum(k):
        drain(r2.at[k], sem2.at[k])
        for h in range(2):
            s2[k, h] = second_total(k, h).astype(BF16)
        remote(s2.at[k], r3.at[k], send3, sem3, (e, z_of(k), l, y, c))

    pick = jnp.where(
        ((g_row >> 1) == iota((128, 256), 0)) & mine_row, 1.0, 0.0
    ).astype(BF16)
    place = jnp.where(
        ((g_col >> 1) == iota((256, 128), 1)) & jnp.logical_not(mine_col), 1.0, 0.0
    ).astype(BF16)
    first = jnp.where(mine_col, ((slot_col >> 2) * 2 + (k_col >> 1)) * 4, -8)
    other_rep = (1 - e, z, l, y, c)

    def compact(r):
        chosen = jnp.where(iota((256, 1024), 1) == first + r, 1.0, 0.0).astype(BF16)
        rows = dot(chosen, recv[...].reshape(1024, 512)).astype(BF16)
        own[r] = rows
        comp[r] = dot(pick, rows).astype(BF16)
        remote(comp.at[r], comp_in.at[r], send_c, sem_c.at[r], other_rep)

    def within(i, lag, count):
        return (i >= lag) & (i < lag + count)

    def steps(i, carry):
        @pl.when(i < NZ)
        def _():
            send_direct(i)

        @pl.when(within(i, LAGS[0], NZ))
        def _():
            relay(i - LAGS[0])

        @pl.when(within(i, LAGS[1], NZ))
        def _():
            first_sum(i - LAGS[1])

        @pl.when(within(i, LAGS[2], NZ - 1))
        def _():
            second_sum(i - LAGS[2])

        @pl.when(i == COMPACT)
        def _():
            drain(recv.at[pl.ds(0, NSH - 1)], sem_a)

        @pl.when(within(i, COMPACT, 4))
        def _():
            compact(i - COMPACT)

        return carry

    lax.fori_loop(0, NZ, multiply, 0)
    lax.fori_loop(AHEAD, max(NZ + LAGS[1], NZ - 1 + LAGS[2]), steps, 0)

    def assemble(r, carry):
        drain(comp_in.at[r], sem_c.at[r])
        up_out[r] = (dot(place, comp_in[r]) + own[r].astype(F32)).astype(BF16)
        return carry

    lax.fori_loop(0, 3, assemble, 0)

    drain(r2.at[NZ - 1], sem2.at[NZ - 1])
    drain(r3, sem3)
    for h in range(2):
        total = second_total(NZ - 1, h)
        for k in range(NZ - 1):
            total = total + r3[k, h].astype(F32)
        fin[h] = total
    here = gk_out.at[:, pl.ds(pl.multiple_of((c * 2 + e) * 256, 256), 256)]
    pltpu.make_async_copy(fin.at[c], here, loc_f).start()
    remote(fin.at[c], here, send_f, sem_f, (1 - e, z, l, y, c))
    remote(fin.at[1 - c], here, send_f, sem_f, (e, z, l, y, 1 - c))
    remote(fin.at[1 - c], here, send_f, sem_f, (1 - e, z, l, y, 1 - c))

    assemble(3, 0)
    drain(fin.at[0], loc_f)
    drain(gk_out.at[:, pl.ds(0, 768)], sem_f)
    drain(gk_out.at[:, pl.ds(0, 768)], send_f)
    drain(kgs.at[my_rows, :], send_key)
    drain(xs.at[:, my_rows, :], send_core)
    drain(rel, send_rel)
    drain(rel, send_dir)
    drain(cmb, send_cmb)
    drain(r2, send2)
    drain(r3, send3)
    drain(recv.at[pl.ds(0, NSH - 1)], send_a)
    drain(comp, send_c)


def shards(tokens_x, key_grad, left_root, slot_grads, right_root, block_slot):
    any_space = pl.BlockSpec(memory_space=pl.ANY)
    vmem = pltpu.VMEM
    dma = pltpu.SemaphoreType.DMA
    return pl.pallas_call(
        kernel,
        out_shape=(
            jax.ShapeDtypeStruct((32, 1024), F32),
            jax.ShapeDtypeStruct((4, 256, 512), BF16),
        ),
        in_specs=[any_space] * 6,
        out_specs=(pl.BlockSpec(memory_space=pltpu.VMEM), pl.BlockSpec(memory_space=pltpu.VMEM)),
        scratch_shapes=[
            vmem((1, 256), jnp.int32),
            vmem((8, 512, 512), BF16),
            vmem((512, 512), BF16),
            vmem((4, 512, 512), BF16),
            vmem((4, 512, 512), BF16),
            vmem((4, 512, 512), BF16),
            vmem((8, 2, 4, 4, 32, 256), BF16),
            vmem((8, 2, 2, 2, 32, 256), BF16),
            vmem((8, 2, 2, 2, 32, 256), BF16),
            vmem((8, 2, 2, 4, 32, 256), BF16),
            vmem((8, 2, 4, 32, 256), BF16),
            vmem((8, 2, 3, 32, 256), BF16),
            vmem((7, 2, 32, 256), BF16),
            vmem((7, 2, 32, 256), BF16),
            vmem((2, 32, 256), F32),
            vmem((128, 8, 512), BF16),
            vmem((128, 8, 512), BF16),
            vmem((4, 256, 512), BF16),
            vmem((4, 128, 512), BF16),
            vmem((4, 128, 512), BF16),
            vmem((4, 256, 512), BF16),
            dma((8,)), dma((8,)), dma((2,)), dma((4,)),
            dma, dma, dma, dma, dma, dma, dma, dma((8,)), dma((8,)), dma((8,)), dma, dma, dma, dma,
            dma, dma, dma, dma((4,)), dma,
        ],
        compiler_params=pltpu.CompilerParams(has_side_effects=True, collective_id=0, vmem_limit_bytes=51 * 2**20),
        cost_estimate=pl.CostEstimate(
            flops=6 * 10**9, bytes_accessed=10 * 2**20, transcendentals=0
        ),
    )(tokens_x, key_grad, left_root, slot_grads, right_root, block_slot.reshape(1, 256))


def solution(mesh):
    finer = Mesh(mesh.devices.reshape(mesh.shape["rep"], 8, 2, 4, 2), AXES)
    in_specs = (
        P(AXES, None),
        P(AXES, None),
        P(SHARD, None, None),
        P(SHARD, None, None),
        P(SHARD, None, None),
        P(),
    )
    out_specs = (P(SHARD, None), P(SHARD, None, None))
    return jax.shard_map(
        shards, mesh=finer, in_specs=in_specs, out_specs=out_specs, check_vma=False
    )
```

```python
import functools

import jax
import jax.numpy as jnp
from jax import lax
from jax.experimental import pallas as pl
from jax.experimental.pallas import tpu as pltpu
from jax.sharding import Mesh
from jax.sharding import PartitionSpec as P

AXES = ("rep", "shard_0", "shard_1", "shard_2", "shard_3")
SHARD = AXES[1:]
MESH = pl.DeviceIdType.MESH
F32 = jnp.float32
BF16 = jnp.bfloat16
NZ, NX, NY = 8, 4, 4
NSH = 128
LAGS = (2, 4, 8)
AHEAD = 2
COMPACT = 7


def dot(a, b):
    return lax.dot_general(a, b, (((1,), (0,)), ((), ())), preferred_element_type=F32)


def dot_t(a, b):
    return lax.dot_general(a, b, (((0,), (0,)), ((), ())), preferred_element_type=F32)


def iota(shape, dim):
    return lax.broadcasted_iota(jnp.int32, shape, dim)


def drain(ref, sem):
    pltpu.make_async_copy(ref, ref, sem).wait()


def kernel(
    x_hbm, kg_hbm, left_hbm, grads_hbm, right_hbm, slot_hbm,
    gk_out, up_out,
    slot_ref, xs, kgs, left_v, grads_v, right_v,
    t1, rel, cmb, r1, s1, r2, s2, r3, fin,
    prod, recv, own, comp, comp_in, upd,
    x_sem, x_rsem, kg_sem, w_sem,
    send_core, send_key, send_rel, send_dir, send_cmb, send2, send3, sem_rel, sem1, sem2, sem3, send_f, sem_f, loc_f,
    send_a, sem_a, send_c, sem_c, out_sem,
):
    e = lax.axis_index("rep")
    z = lax.axis_index("shard_0")
    l = lax.axis_index("shard_1")
    y = lax.axis_index("shard_2")
    c = lax.axis_index("shard_3")
    xp = e * 2 + l
    me = ((z * 2 + l) * 4 + y) * 2 + c
    partner = (e, z, l, y, 1 - c)

    def remote(src, dst, send_sem, recv_sem, device):
        pltpu.make_async_remote_copy(
            src_ref=src, dst_ref=dst, send_sem=send_sem, recv_sem=recv_sem,
            device_id=device, device_id_type=MESH,
        ).start()

    slots = pltpu.make_async_copy(slot_hbm, slot_ref, w_sem.at[3])
    slots.start()
    weights = ((left_hbm, left_v), (grads_hbm, grads_v), (right_hbm, right_v))
    for i, (src, dst) in enumerate(weights):
        pltpu.make_async_copy(src, dst, w_sem.at[i]).start()

    barrier = pltpu.get_barrier_semaphore()

    def peer(k, m):
        tz = lax.rem(z + k + m, NZ)
        return (
            e, tz, lax.rem(l + m % 2, 2), lax.rem(y + m // 2 % 4, 4), lax.rem(c + m // 8, 2)
        )

    def greet(there):
        pl.semaphore_signal(barrier, inc=1, device_id=there, device_id_type=MESH)

    def greet_all(k, carry):
        dz = 4 + (k + 1) // 2 * (1 - 2 * lax.rem(k, 2))
        tz = lax.rem(z + dz, NZ)
        for dy in (2, 1, 3, 0):
            for dl in (1, 0):
                for dc in (1, 0):
                    there = (e, tz, lax.rem(l + dl, 2), lax.rem(y + dy, 4), lax.rem(c + dc, 2))
                    if dy or dl or dc:
                        greet(there)
                    else:

                        @pl.when(k < NZ - 1)
                        def _():
                            greet(there)

        return carry

    for there in ((1 - e, z, l, y, c), (1 - e, z, l, y, 1 - c), (1 - e, z, 1 - l, y, c)):
        greet(there)
    lax.fori_loop(0, NZ, greet_all, 0)

    my_rows = pl.ds(pl.multiple_of(c * 256, 256), 256)

    def key_half(which):
        return kg_hbm.at[:, pl.ds(pl.multiple_of(which * 512, 512), 512)]

    pltpu.make_async_copy(key_half(c), kgs.at[my_rows, :], kg_sem.at[0]).start()

    def z_of(k):
        return lax.rem(z + 1 + k, NZ)

    def x_piece(k):
        return x_hbm.at[:, pl.ds(pl.multiple_of(z_of(k) * 512, 512), 512)]

    def fetch(k, carry):
        pltpu.make_async_copy(x_piece(k), xs.at[k, my_rows, :], x_sem.at[k]).start()
        return carry

    lax.fori_loop(0, NZ, fetch, 0)

    def swap(k, carry):
        remote(x_piece(k), xs.at[k, my_rows, :], send_core, x_rsem.at[k], partner)
        return carry

    slots.wait()
    slot_row = slot_ref[...]
    eye = iota((256, 256), 0) == iota((256, 256), 1)
    row_b = jnp.broadcast_to(slot_row, (256, 256))
    slot_col = jnp.sum(jnp.where(eye, row_b, 0), axis=1, keepdims=True)
    col_b = jnp.broadcast_to(slot_col, (256, 256))
    same = (row_b >> 2) == (col_b >> 2)
    less_r = col_b < row_b
    less_c = row_b < col_b
    g_row = jnp.sum(jnp.where(less_r, 1, 0), axis=0, keepdims=True)
    k_row = jnp.sum(jnp.where(less_r & same, 1, 0), axis=0, keepdims=True)
    g_col = jnp.sum(jnp.where(less_c, 1, 0), axis=1, keepdims=True)
    k_col = jnp.sum(jnp.where(less_c & same, 1, 0), axis=1, keepdims=True)
    mine_row = (g_row & 1) == e
    mine_col = (g_col & 1) == e

    for i in range(2):
        drain(left_v, w_sem.at[i])
    parts = []
    for j in range(2):
        hit = mine_row & ((slot_row >> 2) == me) & ((k_row >> 1) == j)
        s = jnp.sum(jnp.where(hit, slot_row & 3, 0))
        half = dot(left_v[s], grads_v[s]).astype(BF16)
        if j == 0:
            drain(right_v, w_sem.at[2])
        parts.append(dot(half, right_v[s]).astype(BF16))

    out_row = iota((256, 256), 0)
    source = ((out_row >> 2) & 1) * 128 + (out_row >> 3) * 4 + (out_row & 3)
    perm = jnp.where(source == iota((256, 256), 1), 1.0, 0.0).astype(BF16)
    for q in range(4):
        stacked = jnp.concatenate([p[q * 128 : (q + 1) * 128] for p in parts], axis=0)
        moved = dot(perm, stacked).astype(BF16)
        prod[pl.ds(q * 32, 32)] = moved.reshape(32, 8, 512)

    pl.semaphore_wait(barrier, NSH + 2)
    remote(key_half(1 - c), kgs.at[my_rows, :], send_key, kg_sem.at[1], partner)
    lax.fori_loop(0, NZ, swap, 0)

    def y_first(k, h):
        return (k >= 0) if h == 0 else (k < 0)

    def pick2(cond, a, b):
        return a if cond is True else jnp.where(cond, a, b)

    def ring(along_y, p):
        return (
            pick2(along_y, e, p // 2),
            z,
            pick2(along_y, l, lax.rem(p, 2)),
            pick2(along_y, p, y),
            c,
        )

    def other(along_y):
        return False if along_y is True else jnp.logical_not(along_y)

    def pos(along_y):
        if along_y is False:
            return xp
        return pick2(along_y, y, xp)

    def ring_of(along_y, p):
        if along_y is False:
            return (p // 2, z, lax.rem(p, 2), y, c)
        return ring(along_y, p)

    def step_to(p, o):
        return lax.rem(p + o, 4)

    lower, upper = pl.ds(0, 2), pl.ds(2, 2)

    def send_rows(k, m):
        device = peer(k, m)
        _, tz, tl, ty, tc = device
        there = ((tz * 2 + tl) * 4 + ty) * 2 + tc
        remote(prod.at[there], recv.at[me], send_a, sem_a, device)

    def send_all(k, carry):
        @pl.when(k > 0)
        def _():
            send_rows(k, 0)

        for m in range(1, 16):
            send_rows(k, m)
        return carry

    lax.fori_loop(0, NZ, send_all, 0)
    recv[me] = prod[me]

    drain(kgs.at[my_rows, :], kg_sem.at[0])
    drain(kgs.at[my_rows, :], kg_sem.at[1])

    def multiply(k, carry):
        drain(xs.at[k, my_rows, :], x_sem.at[k])
        drain(xs.at[k, my_rows, :], x_rsem.at[k])
        acc = dot_t(xs[k], kgs[...])
        for h in range(2):
            along_y = y_first(k, h)
            for xl in range(2):
                for yy in range(NY):
                    for xe in range(2):
                        base = (xl * 4 + yy) * 64 + h * 32
                        cols = slice(xe * 256, (xe + 1) * 256)
                        xx = xe * 2 + xl
                        piece = acc[base : base + 32, cols].astype(BF16)
                        t1[k, h, pick2(along_y, yy, xx), pick2(along_y, xx, yy)] = piece

        @pl.when(k < AHEAD)
        def _():
            send_direct(k)

        return carry

    def send_direct(k):
        for h in range(2):
            along_y = y_first(k, h)
            p = pos(along_y)
            nxt, far, prv = step_to(p, 1), step_to(p, 2), step_to(p, 3)
            to_n, to_p = ring_of(along_y, nxt), ring_of(along_y, prv)
            remote(t1.at[k, h, far, lower], rel.at[k, h, 0], send_rel, sem_rel.at[k], to_n)
            remote(t1.at[k, h, far, upper], rel.at[k, h, 1], send_rel, sem_rel.at[k], to_p)
            remote(t1.at[k, h, nxt, upper], r1.at[k, h, 0, upper], send_dir, sem1.at[k], to_n)
            remote(t1.at[k, h, prv, lower], r1.at[k, h, 1, lower], send_dir, sem1.at[k], to_p)

    def relay(k):
        drain(rel.at[k], sem_rel.at[k])
        for h in range(2):
            along_y = y_first(k, h)
            p = pos(along_y)
            nxt, prv = step_to(p, 1), step_to(p, 3)
            half = t1[k, h, nxt, 0:2].astype(F32) + rel[k, h, 0].astype(F32)
            cmb[k, h, 0] = half.astype(BF16)
            remote(cmb.at[k, h, 0], r1.at[k, h, 0, lower], send_cmb, sem1.at[k], ring_of(along_y, nxt))
            half = t1[k, h, prv, 2:4].astype(F32) + rel[k, h, 1].astype(F32)
            cmb[k, h, 1] = half.astype(BF16)
            remote(cmb.at[k, h, 1], r1.at[k, h, 1, upper], send_cmb, sem1.at[k], ring_of(along_y, prv))

    def first_sum(k):
        drain(r1.at[k], sem1.at[k])
        for h in range(2):
            along_y = y_first(k, h)
            total = t1[k, h, pos(along_y)].astype(F32)
            s1[k, h] = (total + r1[k, h, 0].astype(F32) + r1[k, h, 1].astype(F32)).astype(BF16)
        for h in range(2):
            along_y = other(y_first(k, h))
            p = pos(along_y)
            for o in (2, 1, 3):
                to = step_to(p, o)
                remote(s1.at[k, h, to], r2.at[k, h, o - 1], send2, sem2.at[k], ring_of(along_y, to))

    def second_total(k, h):
        total = s1[k, h, pos(other(y_first(k, h)))].astype(F32)
        for o in range(3):
            total = total + r2[k, h, o].astype(F32)
        return total

    def second_sum(k):
        drain(r2.at[k], sem2.at[k])
        for h in range(2):
            s2[k, h] = second_total(k, h).astype(BF16)
        remote(s2.at[k], r3.at[k], send3, sem3, (e, z_of(k), l, y, c))

    pick = jnp.where(
        ((g_row >> 1) == iota((128, 256), 0)) & mine_row, 1.0, 0.0
    ).astype(BF16)
    place = jnp.where(
        ((g_col >> 1) == iota((256, 128), 1)) & jnp.logical_not(mine_col), 1.0, 0.0
    ).astype(BF16)
    first = jnp.where(mine_col, ((slot_col >> 2) * 2 + (k_col >> 1)) * 4, -8)
    other_rep = (1 - e, z, l, y, c)

    def compact(r):
        chosen = jnp.where(iota((256, 1024), 1) == first + r, 1.0, 0.0).astype(BF16)
        rows = dot(chosen, recv[...].reshape(1024, 512)).astype(BF16)
        own[r] = rows
        comp[r] = dot(pick, rows).astype(BF16)
        remote(comp.at[r], comp_in.at[r], send_c, sem_c.at[r], other_rep)

    def within(i, lag, count):
        return (i >= lag) & (i < lag + count)

    def steps(i, carry):
        @pl.when(within(i, LAGS[0], NZ))
        def _():
            relay(i - LAGS[0])

        @pl.when(i < NZ)
        def _():
            send_direct(i)

        @pl.when(within(i, LAGS[1], NZ))
        def _():
            first_sum(i - LAGS[1])

        @pl.when(within(i, LAGS[2], NZ - 1))
        def _():
            second_sum(i - LAGS[2])

        @pl.when(i == COMPACT)
        def _():
            drain(recv.at[pl.ds(0, NSH - 1)], sem_a)

        @pl.when(within(i, COMPACT, 4))
        def _():
            compact(i - COMPACT)

        return carry

    lax.fori_loop(0, NZ, multiply, 0)
    lax.fori_loop(AHEAD, max(NZ + LAGS[1], NZ - 1 + LAGS[2]), steps, 0)

    def assemble(r, carry):
        drain(comp_in.at[r], sem_c.at[r])
        up_out[r] = (dot(place, comp_in[r]) + own[r].astype(F32)).astype(BF16)
        return carry

    lax.fori_loop(0, 3, assemble, 0)

    drain(r2.at[NZ - 1], sem2.at[NZ - 1])
    drain(r3, sem3)
    for h in range(2):
        total = second_total(NZ - 1, h)
        for k in range(NZ - 1):
            total = total + r3[k, h].astype(F32)
        fin[h] = total
    here = gk_out.at[:, pl.ds(pl.multiple_of((c * 2 + e) * 256, 256), 256)]
    remote(fin.at[1 - c], here, send_f, sem_f, (1 - e, z, l, y, 1 - c))
    remote(fin.at[c], here, send_f, sem_f, (1 - e, z, l, y, c))
    remote(fin.at[1 - c], here, send_f, sem_f, (e, z, l, y, 1 - c))
    pltpu.make_async_copy(fin.at[c], here, loc_f).start()

    assemble(3, 0)
    drain(fin.at[0], loc_f)
    drain(gk_out.at[:, pl.ds(0, 768)], sem_f)
    drain(gk_out.at[:, pl.ds(0, 768)], send_f)
    drain(kgs.at[my_rows, :], send_key)
    drain(xs.at[:, my_rows, :], send_core)
    drain(rel, send_rel)
    drain(rel, send_dir)
    drain(cmb, send_cmb)
    drain(r2, send2)
    drain(r3, send3)
    drain(recv.at[pl.ds(0, NSH - 1)], send_a)
    drain(comp, send_c)


def shards(tokens_x, key_grad, left_root, slot_grads, right_root, block_slot):
    any_space = pl.BlockSpec(memory_space=pl.ANY)
    vmem = pltpu.VMEM
    dma = pltpu.SemaphoreType.DMA
    return pl.pallas_call(
        kernel,
        out_shape=(
            jax.ShapeDtypeStruct((32, 1024), F32),
            jax.ShapeDtypeStruct((4, 256, 512), BF16),
        ),
        in_specs=[any_space] * 6,
        out_specs=(pl.BlockSpec(memory_space=pltpu.VMEM), pl.BlockSpec(memory_space=pltpu.VMEM)),
        scratch_shapes=[
            vmem((1, 256), jnp.int32),
            vmem((8, 512, 512), BF16),
            vmem((512, 512), BF16),
            vmem((4, 512, 512), BF16),
            vmem((4, 512, 512), BF16),
            vmem((4, 512, 512), BF16),
            vmem((8, 2, 4, 4, 32, 256), BF16),
            vmem((8, 2, 2, 2, 32, 256), BF16),
            vmem((8, 2, 2, 2, 32, 256), BF16),
            vmem((8, 2, 2, 4, 32, 256), BF16),
            vmem((8, 2, 4, 32, 256), BF16),
            vmem((8, 2, 3, 32, 256), BF16),
            vmem((7, 2, 32, 256), BF16),
            vmem((7, 2, 32, 256), BF16),
            vmem((2, 32, 256), F32),
            vmem((128, 8, 512), BF16),
            vmem((128, 8, 512), BF16),
            vmem((4, 256, 512), BF16),
            vmem((4, 128, 512), BF16),
            vmem((4, 128, 512), BF16),
            vmem((4, 256, 512), BF16),
            dma((8,)), dma((8,)), dma((2,)), dma((4,)),
            dma, dma, dma, dma, dma, dma, dma, dma((8,)), dma((8,)), dma((8,)), dma, dma, dma, dma,
            dma, dma, dma, dma((4,)), dma,
        ],
        compiler_params=pltpu.CompilerParams(has_side_effects=True, collective_id=0, vmem_limit_bytes=51 * 2**20),
        cost_estimate=pl.CostEstimate(
            flops=6 * 10**9, bytes_accessed=10 * 2**20, transcendentals=0
        ),
    )(tokens_x, key_grad, left_root, slot_grads, right_root, block_slot.reshape(1, 256))


def solution(mesh):
    finer = Mesh(mesh.devices.reshape(mesh.shape["rep"], 8, 2, 4, 2), AXES)
    in_specs = (
        P(AXES, None),
        P(AXES, None),
        P(SHARD, None, None),
        P(SHARD, None, None),
        P(SHARD, None, None),
        P(),
    )
    out_specs = (P(SHARD, None), P(SHARD, None, None))
    return jax.shard_map(
        shards, mesh=finer, in_specs=in_specs, out_specs=out_specs, check_vma=False
    )
```
